32 devices in a mesh: tok: 4 (over y, x), hid: 2 (over core), voc: 4 (over z).
Axes of the slice: x: 2, y: 2, z: 4, core: 2. Of those that a mesh axis runs over, the one named last changes fastest.
Arguments:
- student_hidden: bfloat16 [512, 8192], P('tok', ('hid', 'voc')), may hold values from -8 to 8
- teacher_hidden: bfloat16 [512, 16384], P('tok', ('hid', 'voc')), may hold values from -8 to 8
- student_head: bfloat16 [8192, 2048], P('hid', 'voc'), may hold values from -2 to 2
- teacher_head: bfloat16 [16384, 2048], P('hid', 'voc'), may hold values from -2 to 2
- loss_weight: float32 [512], P('tok'), may hold values from 128 to 1024
Outputs:
- grad_hidden: bfloat16 [512, 8192], P('tok', ('hid', 'voc'))
- mean_loss: float32 [], replicated
The draws below stay inside these ranges and needn't reach their ends.
All inputs are finite; a program needn't handle non-finite values.
Results may differ from the reference program's by a relative error of at most 0.001.
The reference program's roundings to bfloat16 on the way (of `scaled_gap`) count: a program that leaves them out, or rounds other values in their place, can miss the bound.
Values may be sent and summed in bfloat16 or wider, within the bound.
A program may use at most 64 MiB of HBM per device.

```python
import math
import jax
import jax.numpy as jnp

DS = 8192
DT = 16384
TOKENS = 512
V = 2048


def head_values(key, width, salt):
    values = jax.random.normal(jax.random.fold_in(key, salt), (width, V), jnp.float32)
    return jnp.clip(values, -5.0, 5.0) * (2.0 / math.sqrt(width))


def hidden_values(key, width, head_salt, salt):
    values = jnp.clip(jax.random.normal(jax.random.fold_in(key, salt), (TOKENS, width), jnp.float32), -6.0, 6.0)
    return values


def draw_student_head(key, part):
    return head_values(key, DS, 11).astype(jnp.bfloat16)


def draw_teacher_head(key, part):
    return head_values(key, DT, 12).astype(jnp.bfloat16)


def draw_student_hidden(key, part):
    return hidden_values(key, DS, 11, 13).astype(jnp.bfloat16)


def draw_teacher_hidden(key, part):
    return hidden_values(key, DT, 12, 14).astype(jnp.bfloat16)


def block_levels(stream_key, shape, pieces, least, high):
    level = 1.0
    for dim, blocks in pieces:
        steps = jax.random.uniform(jax.random.fold_in(jax.random.fold_in(stream_key, 6), dim), (blocks,), jnp.float32, least / len(pieces), high / len(pieces))
        level = level * jnp.repeat(jnp.exp(steps), shape[dim] // blocks).reshape((-1,) + (1,) * (len(shape) - 1 - dim))
    return level


def setup_inputs(seed: int = 0) -> dict:
    key_of = jax.random.split(jax.random.key(seed), 6)
    return {
        "student_hidden": draw_student_hidden(jax.random.fold_in(key_of[5], 71), 0),
        "teacher_hidden": draw_teacher_hidden(jax.random.fold_in(key_of[5], 71), 0),
        "student_head": draw_student_head(jax.random.fold_in(key_of[5], 71), 0),
        "teacher_head": draw_teacher_head(jax.random.fold_in(key_of[5], 71), 0),
        "loss_weight": jnp.clip(jnp.exp(math.log(1024.0) - 2.0794415 * jax.random.uniform(key_of[4], (TOKENS,), jnp.float32) ** block_levels(key_of[4], (TOKENS,), ((0, 4),), -0.2, 0.2)), 128.0, 1024.0),
    }


def reference(student_hidden, teacher_hidden, student_head, teacher_head, loss_weight):
    student_logits = jnp.dot(student_hidden, student_head, preferred_element_type=jnp.float32)
    teacher_logits = jnp.dot(teacher_hidden, teacher_head, preferred_element_type=jnp.float32)
    student_peak = jnp.max(student_logits, axis=1)
    teacher_peak = jnp.max(teacher_logits, axis=1)
    student_lse = student_peak + jnp.log(jnp.sum(jnp.exp(student_logits - student_peak[:, None]), axis=1))
    teacher_lse = teacher_peak + jnp.log(jnp.sum(jnp.exp(teacher_logits - teacher_peak[:, None]), axis=1))
    teacher_prob = jnp.exp(teacher_logits - teacher_lse[:, None])
    student_prob = jnp.exp(student_logits - student_lse[:, None])
    divergence = jnp.sum(teacher_prob * (teacher_logits - student_logits), axis=1) - teacher_lse + student_lse
    mean_loss = jnp.sum(divergence) / TOKENS
    scaled_gap = (loss_weight[:, None] * (student_prob - teacher_prob)).astype(jnp.bfloat16)
    grad_hidden = jax.lax.dot_general(scaled_gap, student_head, (((1,), (1,)), ((), ())), preferred_element_type=jnp.float32)
    return grad_hidden.astype(jnp.bfloat16), mean_loss
```

```python
import functools

import jax
import jax.numpy as jnp
from jax import lax
from jax.experimental import pallas as pl
from jax.experimental.pallas import tpu as pltpu
from jax.sharding import PartitionSpec as P

MESH = pl.DeviceIdType.MESH
F32 = jnp.float32
BF16 = jnp.bfloat16


def fused(n, nt, x_ref, y_ref, w_ref, sw_hbm, tw_hbm, out, loss_out,
          wf, tw, tg, sp, spx, ssum, srr, tacc, tpx, stat, gap, wcol, lossb, acc,
          lc, wz_s, wz_r, wt_s, wt_r, th_s, th_r, px_s, px_r, rs_s, rs_r,
          st_s, st_r, gz_s, gz_r, gx_s, gx_r, ls_s, ls_r):
    z = lax.axis_index("voc")
    t = lax.axis_index("tok")
    h = lax.axis_index("hid")
    rows, ks = x_ref.shape
    kt = y_ref.shape[1]
    half = rows // 2
    quarter = ks // nt
    partner = {"hid": 1 - h}
    mine = pl.ds(pl.multiple_of(h * half, half), half)
    theirs = pl.ds(pl.multiple_of((1 - h) * half, half), half)
    me = t * 2 + h

    def rc(src, dst, ss, rs, dev):
        return pltpu.make_async_remote_copy(
            src_ref=src, dst_ref=dst, send_sem=ss, recv_sem=rs,
            device_id=dev, device_id_type=MESH)

    def zdev(k):
        return lax.rem(z + k, n)

    plane = []
    for q in range(nt):
        for c in range(2):
            if q or c:
                plane.append((lax.rem(t + q, nt), lax.rem(h + c, 2)))

    own_w = pltpu.make_async_copy(sw_hbm.at[pl.ds(pl.multiple_of(z * ks, ks), ks)], wf.at[z], lc.at[n])
    own_w.start()

    def tw_copy(i):
        return pltpu.make_async_copy(tw_hbm.at[pl.ds(pl.multiple_of(i * kt, kt), kt)], tw.at[i], lc.at[i])

    barrier = pltpu.get_barrier_semaphore()
    for k in range(1, n):
        pl.semaphore_signal(barrier, inc=1, device_id={"voc": zdev(k)}, device_id_type=MESH)
    for (a, b) in plane:
        pl.semaphore_signal(barrier, inc=1, device_id={"tok": a, "hid": b}, device_id_type=MESH)
    pl.semaphore_wait(barrier, n - 1 + len(plane))

    def part(i):
        return pl.ds(pl.multiple_of(i * quarter, quarter), quarter)

    def wz(j):
        return rc(sw_hbm.at[pl.ds(pl.multiple_of(j * ks + t * quarter, quarter), quarter)],
                  wf.at[z, part(t)], wz_s.at[j], wz_r.at[z], {"voc": j})

    def wz_in(j):
        return rc(wf.at[j, part(t)], wf.at[j, part(t)], wz_s.at[j], wz_r.at[j], {"voc": j})

    def wt(j, dst_t):
        return rc(wf.at[j, part(t)], wf.at[j, part(t)], wt_s.at[j, dst_t], wt_r.at[j, t], {"tok": dst_t})

    def wt_in(j, src_t):
        return rc(wf.at[j, part(src_t)], wf.at[j, part(src_t)], wt_s.at[j, src_t], wt_r.at[j, src_t], {"tok": src_t})

    def sides(d):
        return ((z - d, z - d >= 0), (z + d, z + d < n))

    for d in range(1, n):
        for j, ok in sides(d):
            @pl.when(ok)
            def _(j=j):
                wz(j).start()

    def piece(r):
        return pl.ds(r * half, half)

    def own_y(r, side):
        return rc(y_ref.at[piece(r)], tg.at[z, piece(r)], th_s.at[side, z, r], th_r.at[z, r],
                  {"voc": z + (1 if side else -1)})

    def relay_y(i, r, side):
        return rc(tg.at[i, piece(r)], tg.at[i, piece(r)], th_s.at[side, i, r], th_r.at[i, r],
                  {"voc": z + (1 if side else -1)})

    room = (z - 1 >= 0, z + 1 < n)
    for r in range(2):
        for side in range(2):
            @pl.when(room[side])
            def _(r=r, side=side):
                own_y(r, side).start()

    for k in range(n):
        tw_copy(zdev(k)).start()

    wcol[...] = jnp.transpose(jnp.broadcast_to(w_ref[...], (rows, rows)))

    for d in range(1, n):
        for j, ok in sides(d):
            @pl.when(ok)
            def _(j=j):
                wz_in(j).wait_recv()
                for q in range(1, nt):
                    wt(j, lax.rem(t + q, nt)).start()

    def teacher_dot(src, i, first):
        tw_copy(i).wait()
        step = kt // 2

        @pl.loop(0, 2)
        def _(s):
            cols = pl.ds(pl.multiple_of(s * step, step), step)
            term = jnp.dot(src[:, cols], tw[i, cols, :], preferred_element_type=F32)
            if first:
                @pl.when(s == 0)
                def _():
                    tacc[...] = term

                @pl.when(s > 0)
                def _():
                    tacc[...] += term
            else:
                tacc[...] += term

    teacher_dot(y_ref, z, True)

    def take_y(d, dot):
        for r in range(2):
            for side, (i, ok) in enumerate(sides(d)):
                @pl.when(ok)
                def _(i=i, side=side, r=r):
                    relay_y(i, r, side).wait_recv()
                    if d < n - 1:
                        on = 1 - side

                        @pl.when(room[on])
                        def _():
                            relay_y(i, r, on).start()
        if dot:
            dot_y(d)

    def dot_y(d):
        for i, ok in sides(d):
            @pl.when(ok)
            def _(i=i):
                teacher_dot(tg.at[i], i, False)

    def student(k):
        j = zdev(k)
        if k == 0:
            own_w.wait()
        else:
            for q in range(1, nt):
                wt_in(j, lax.rem(t + q, nt)).wait_recv()
        sp[j] = jnp.dot(x_ref[...], wf[j], preferred_element_type=F32)
        rc(sp.at[j, theirs], spx.at[j], px_s.at[j], px_r.at[j], partner).start()

    def student_send(k):
        j = zdev(k)
        rc(sp.at[j, theirs], spx.at[j], px_s.at[j], px_r.at[j], partner).wait_recv()
        ssum[j] = sp[j, mine, :] + spx[j]
        if k:
            rc(ssum.at[j], srr.at[z], rs_s.at[j], rs_r.at[z], {"voc": j}).start()

    student(0)
    for d in range(1, n - 1):
        take_y(d, True)
    student_send(0)
    for k in range(1, n):
        student(k)
        student_send(k)
    take_y(n - 1, True)

    tx = rc(tacc.at[theirs], tpx, px_s.at[n], px_r.at[n], partner)
    tx.start()
    sl = ssum[z]
    for k in range(1, n):
        j = zdev(k)
        rc(srr.at[j], srr.at[j], rs_s.at[j], rs_r.at[j], {"voc": j}).wait_recv()
        sl = sl + srr[j]
    ssum[z] = sl
    ms = jnp.max(sl, axis=1, keepdims=True)
    ss = jnp.sum(jnp.exp(sl - ms), axis=1, keepdims=True)
    tx.wait_recv()
    tl = tacc[mine, :] + tpx[...]
    tpx[...] = tl
    mt = jnp.max(tl, axis=1, keepdims=True)
    et = jnp.exp(tl - mt)
    st = jnp.sum(et, axis=1, keepdims=True)
    cr = jnp.sum(et * (tl - sl), axis=1, keepdims=True)
    lane = lax.broadcasted_iota(jnp.int32, (half, 128), 1)
    stat[z] = jnp.where(lane == 0, ms, jnp.where(lane == 1, mt, jnp.where(
        lane == 2, ss, jnp.where(lane == 3, st, cr))))

    def stx(j, src):
        return rc(stat.at[src], stat.at[src], st_s.at[j], st_r.at[src], {"voc": j})

    for k in range(1, n):
        stx(zdev(k), z).start()
    for k in range(1, n):
        stx(zdev(k), zdev(k)).wait_recv()
    parts = [stat[j] for j in range(n)]
    top = parts[0]
    for p in parts[1:]:
        top = jnp.maximum(top, p)
    big_s, big_t = top[:, 0:1], top[:, 1:2]
    tot_s = jnp.zeros_like(big_s)
    tot_t = jnp.zeros_like(big_s)
    cross = jnp.zeros_like(big_s)
    for p in parts:
        es = jnp.exp(p[:, 0:1] - big_s)
        ets = jnp.exp(p[:, 1:2] - big_t)
        tot_s = tot_s + p[:, 2:3] * es
        tot_t = tot_t + p[:, 3:4] * ets
        cross = cross + p[:, 4:5] * ets
    lse_s = big_s + jnp.log(tot_s)
    lse_t = big_t + jnp.log(tot_t)
    scale = wcol[mine, :][:, 0:1]
    gap[z, mine, :] = (scale * (jnp.exp(ssum[z] - lse_s) - jnp.exp(tpx[...] - lse_t))).astype(BF16)

    def gz(j, src):
        return rc(gap.at[src, mine], gap.at[src, mine], gz_s.at[j], gz_r.at[src], {"voc": j})

    def gx(src, side):
        return rc(gap.at[src, side], gap.at[src, side], gx_s.at[src], gx_r.at[src], partner)

    for d in range(1, n):
        for j, ok in sides(d):
            @pl.when(ok)
            def _(j=j):
                gz(j, z).start()
    gx(z, mine).start()

    div = cross / tot_t - lse_t + lse_s
    lossb[me] = jnp.broadcast_to(jnp.sum(div, axis=0, keepdims=True), (8, 128))

    def ls(a, b, src):
        return rc(lossb.at[src], lossb.at[src], ls_s.at[a * 2 + b], ls_r.at[src], {"tok": a, "hid": b})

    for (a, b) in plane:
        ls(a, b, me).start()

    def grad_dot(j, first):
        term = lax.dot_general(gap[j], wf[j], (((1,), (1,)), ((), ())), preferred_element_type=F32)
        if first:
            acc[...] = term
        else:
            acc[...] += term

    gx(z, theirs).wait_recv()
    grad_dot(z, True)
    for d in range(1, n):
        for j, ok in sides(d):
            @pl.when(ok)
            def _(j=j):
                gz(j, j).wait_recv()
                gx(j, mine).start()
    for k in range(1, n):
        j = zdev(k)
        gx(j, theirs).wait_recv()
        grad_dot(j, False)
    out[...] = acc[...].astype(BF16)

    for (a, b) in plane:
        ls(a, b, a * 2 + b).wait_recv()
    total = lossb[0]
    for p in range(1, nt * 2):
        total = total + lossb[p]
    loss_out[0, 0] = total[0, 0] / (rows * nt)

    for k in range(1, n):
        j = zdev(k)
        wz(j).wait_send()
        for q in range(1, nt):
            wt(j, lax.rem(t + q, nt)).wait_send()
        rc(ssum.at[j], srr.at[z], rs_s.at[j], rs_r.at[z], {"voc": j}).wait_send()
        stx(j, z).wait_send()
        gz(j, z).wait_send()
    for r in range(2):
        for side in range(2):
            @pl.when(room[side])
            def _(r=r, side=side):
                own_y(r, side).wait_send()
    for d in range(1, n - 1):
        for r in range(2):
            for side, (i, ok) in enumerate(sides(d)):
                on = 1 - side

                @pl.when(jnp.logical_and(ok, room[on]))
                def _(i=i, r=r, on=on):
                    relay_y(i, r, on).wait_send()
    for k in range(n):
        j = zdev(k)
        rc(sp.at[j, theirs], spx.at[j], px_s.at[j], px_r.at[j], partner).wait_send()
        gx(j, mine).wait_send()
    tx.wait_send()
    for (a, b) in plane:
        ls(a, b, me).wait_send()


def fused_shards(n, nt, student_hidden, teacher_hidden, student_head, teacher_head, loss_weight):
    rows, ks = student_hidden.shape
    kt = teacher_hidden.shape[1]
    v = student_head.shape[1]
    half = rows // 2
    dma = lambda *s: pltpu.SemaphoreType.DMA(s)
    vmem = lambda s, d: pltpu.VMEM(s, d)
    whole = pl.BlockSpec(memory_space=pltpu.VMEM)
    anywhere = pl.BlockSpec(memory_space=pl.ANY)
    grad, loss = pl.pallas_call(
        functools.partial(fused, n, nt),
        out_shape=(jax.ShapeDtypeStruct((rows, ks), BF16), jax.ShapeDtypeStruct((1, 1), F32)),
        in_specs=[whole, whole, whole, anywhere, anywhere],
        out_specs=(whole, pl.BlockSpec(memory_space=pltpu.SMEM)),
        scratch_shapes=[
            vmem((n, ks, v), BF16),
            vmem((n, kt, v), BF16),
            vmem((n, rows, kt), BF16),
            vmem((n, rows, v), F32),
            vmem((n, half, v), F32),
            vmem((n, half, v), F32),
            vmem((n, half, v), F32),
            vmem((rows, v), F32),
            vmem((half, v), F32),
            vmem((n, half, 128), F32),
            vmem((n, rows, v), BF16),
            vmem((rows, rows), F32),
            vmem((nt * 2, 8, 128), F32),
            vmem((rows, ks), F32),
            dma(n + 1),
            dma(n), dma(n), dma(n, nt), dma(n, nt),
            dma(2, n, 2), dma(n, 2),
            dma(n + 1), dma(n + 1), dma(n), dma(n),
            dma(n), dma(n), dma(n), dma(n), dma(n), dma(n),
            dma(nt * 2), dma(nt * 2),
        ],
        compiler_params=pltpu.CompilerParams(
            collective_id=0, has_side_effects=True, vmem_limit_bytes=48 << 20),
        name="divergence_grad",
    )(student_hidden, teacher_hidden, loss_weight.reshape(1, rows), student_head, teacher_head)
    return grad, loss.reshape(())


def divergence_terms(student_logits, teacher_logits, weights):
    differences = teacher_logits - student_logits
    peak_student, peak_teacher = lax.pmax(
        (jnp.max(student_logits, axis=1), jnp.max(teacher_logits, axis=1)), "voc"
    )
    scaled_student = jnp.exp(student_logits - peak_student[:, None])
    scaled_teacher = jnp.exp(teacher_logits - peak_teacher[:, None])
    total_student, total_teacher, cross_sum = lax.psum(
        (
            jnp.sum(scaled_student, axis=1),
            jnp.sum(scaled_teacher, axis=1),
            jnp.sum(scaled_teacher * differences, axis=1),
        ),
        "voc",
    )
    student_lse = peak_student + jnp.log(total_student)
    teacher_lse = peak_teacher + jnp.log(total_teacher)
    divergence = cross_sum / total_teacher - teacher_lse + student_lse
    prob_gap = jnp.exp(student_logits - student_lse[:, None]) - jnp.exp(
        teacher_logits - teacher_lse[:, None]
    )
    scaled_gap = (weights[:, None] * prob_gap).astype(jnp.bfloat16)
    return (divergence, scaled_gap)


def plain_shards(student_hidden, teacher_hidden, student_head, teacher_head, loss_weight):
    student_block, teacher_block = (
        lax.all_gather(student_hidden, "voc", axis=1, tiled=True),
        lax.all_gather(teacher_hidden, "voc", axis=1, tiled=True),
    )
    vocab_local = student_head.shape[1]
    row_count = student_block.shape[0] // lax.axis_size("hid")
    joined = lax.psum_scatter(
        jnp.concatenate(
            [
                jnp.dot(student_block, student_head, preferred_element_type=jnp.float32),
                jnp.dot(teacher_block, teacher_head, preferred_element_type=jnp.float32),
            ],
            axis=1,
        ),
        "hid",
        scatter_dimension=0,
        tiled=True,
    )
    student_logits = joined[:, :vocab_local]
    teacher_logits = joined[:, vocab_local:]
    weights = lax.dynamic_slice_in_dim(loss_weight, lax.axis_index("hid") * row_count, row_count)
    divergence, scaled_gap = divergence_terms(student_logits, teacher_logits, weights)
    token_total = loss_weight.shape[0] * lax.axis_size("tok")
    loss_total = lax.psum(jnp.sum(divergence), ("tok", "hid"))
    grad_terms = lax.dot_general(
        lax.all_gather(scaled_gap, "hid", axis=0, tiled=True),
        student_head,
        (((1,), (1,)), ((), ())),
        preferred_element_type=jnp.float32,
    )
    grad_hidden = lax.psum_scatter(grad_terms, "voc", scatter_dimension=1, tiled=True).astype(
        jnp.bfloat16
    )
    mean_loss = loss_total / token_total
    return (grad_hidden, mean_loss)


def solution(mesh):
    placed = (
        P("tok", ("hid", "voc")),
        P("tok", ("hid", "voc")),
        P("hid", "voc"),
        P("hid", "voc"),
        P("tok"),
    )
    n, nt = mesh.shape["voc"], mesh.shape["tok"]
    if n <= 4 and mesh.shape["hid"] == 2:
        body = functools.partial(fused_shards, n, nt)
    else:
        body = plain_shards
    return jax.shard_map(
        body,
        mesh=mesh,
        in_specs=placed,
        out_specs=(P("tok", ("hid", "voc")), P()),
        check_vma=False,
    )
```

```python
import functools

import jax
import jax.numpy as jnp
from jax import lax
from jax.experimental import pallas as pl
from jax.experimental.pallas import tpu as pltpu
from jax.sharding import PartitionSpec as P

MESH = pl.DeviceIdType.MESH
F32 = jnp.float32
BF16 = jnp.bfloat16


def fused(n, nt, x_hbm, y_hbm, w_hbm, sw_hbm, tw_hbm, out, loss_out,
          x_ref, y_ref, w_ref, wf, tw, tg, sp, spx, ssum, srr, tacc, tpx, stat, gap, wcol, lossb, acc,
          lc, wz_s, wz_r, wt_s, wt_r, th_s, th_r, px_s, px_r, rs_s, rs_r,
          st_s, st_r, gz_s, gz_r, gx_s, gx_r, ls_s, ls_r):
    z = lax.axis_index("voc")
    t = lax.axis_index("tok")
    h = lax.axis_index("hid")
    rows, ks = x_ref.shape
    kt = y_ref.shape[1]
    half = rows // 2
    quarter = ks // nt
    partner = {"hid": 1 - h}
    mine = pl.ds(pl.multiple_of(h * half, half), half)
    theirs = pl.ds(pl.multiple_of((1 - h) * half, half), half)
    me = t * 2 + h

    def rc(src, dst, ss, rs, dev):
        return pltpu.make_async_remote_copy(
            src_ref=src, dst_ref=dst, send_sem=ss, recv_sem=rs,
            device_id=dev, device_id_type=MESH)

    def zdev(k):
        return lax.rem(z + k, n)

    plane = []
    for q in range(nt):
        for c in range(2):
            if q or c:
                plane.append((lax.rem(t + q, nt), lax.rem(h + c, 2)))

    own_w = pltpu.make_async_copy(sw_hbm.at[pl.ds(pl.multiple_of(z * ks, ks), ks)], wf.at[z], lc.at[n])
    own_w.start()
    ins = [pltpu.make_async_copy(a, b, lc.at[n + 1 + i])
           for i, (a, b) in enumerate(((x_hbm, x_ref), (y_hbm, y_ref), (w_hbm, w_ref)))]
    for c in ins:
        c.start()

    def tw_copy(i):
        return pltpu.make_async_copy(tw_hbm.at[pl.ds(pl.multiple_of(i * kt, kt), kt)], tw.at[i], lc.at[i])

    barrier = pltpu.get_barrier_semaphore()
    for k in range(1, n):
        pl.semaphore_signal(barrier, inc=1, device_id={"voc": zdev(k)}, device_id_type=MESH)
    for (a, b) in plane:
        pl.semaphore_signal(barrier, inc=1, device_id={"tok": a, "hid": b}, device_id_type=MESH)
    pl.semaphore_wait(barrier, n - 1 + len(plane))

    def part(i):
        return pl.ds(pl.multiple_of(i * quarter, quarter), quarter)

    def wz(j):
        return rc(sw_hbm.at[pl.ds(pl.multiple_of(j * ks + t * quarter, quarter), quarter)],
                  wf.at[z, part(t)], wz_s.at[j], wz_r.at[z], {"voc": j})

    def wz_in(j):
        return rc(wf.at[j, part(t)], wf.at[j, part(t)], wz_s.at[j], wz_r.at[j], {"voc": j})

    def wt(j, dst_t):
        return rc(wf.at[j, part(t)], wf.at[j, part(t)], wt_s.at[j, dst_t], wt_r.at[j, t], {"tok": dst_t})

    def wt_in(j, src_t):
        return rc(wf.at[j, part(src_t)], wf.at[j, part(src_t)], wt_s.at[j, src_t], wt_r.at[j, src_t], {"tok": src_t})

    def sides(d):
        return ((z - d, z - d >= 0), (z + d, z + d < n))

    for d in range(n - 1, 0, -1):
        for j, ok in sides(d):
            @pl.when(ok)
            def _(j=j):
                wz(j).start()

    def piece(r):
        return pl.ds(r * half, half)

    def own_y(r, side):
        return rc(y_hbm.at[piece(r)], tg.at[z, piece(r)], th_s.at[side, z, r], th_r.at[z, r],
                  {"voc": z + (1 if side else -1)})

    def relay_y(i, r, side):
        return rc(tg.at[i, piece(r)], tg.at[i, piece(r)], th_s.at[side, i, r], th_r.at[i, r],
                  {"voc": z + (1 if side else -1)})

    room = (z - 1 >= 0, z + 1 < n)
    for r in range(2):
        for side in range(2):
            @pl.when(room[side])
            def _(r=r, side=side):
                own_y(r, side).start()

    for k in range(n):
        tw_copy(zdev(k)).start()

    for c in ins:
        c.wait()
    wcol[...] = jnp.transpose(jnp.broadcast_to(w_ref[...], (rows, rows)))

    for d in range(n - 1, 0, -1):
        for j, ok in sides(d):
            @pl.when(ok)
            def _(j=j):
                wz_in(j).wait_recv()
                for q in range(1, nt):
                    wt(j, lax.rem(t + q, nt)).start()

    def teacher_dot(src, i, first):
        tw_copy(i).wait()
        step = kt // 2

        @pl.loop(0, 2)
        def _(s):
            cols = pl.ds(pl.multiple_of(s * step, step), step)
            term = jnp.dot(src[:, cols], tw[i, cols, :], preferred_element_type=F32)
            if first:
                @pl.when(s == 0)
                def _():
                    tacc[...] = term

                @pl.when(s > 0)
                def _():
                    tacc[...] += term
            else:
                tacc[...] += term

    teacher_dot(y_ref, z, True)

    def take_y(d, dot):
        for r in range(2):
            for side, (i, ok) in enumerate(sides(d)):
                @pl.when(ok)
                def _(i=i, side=side, r=r):
                    relay_y(i, r, side).wait_recv()
                    if d < n - 1:
                        on = 1 - side

                        @pl.when(room[on])
                        def _():
                            relay_y(i, r, on).start()
        if dot:
            dot_y(d)

    def dot_y(d):
        for i, ok in sides(d):
            @pl.when(ok)
            def _(i=i):
                teacher_dot(tg.at[i], i, False)

    def student(j, own):
        if own:
            own_w.wait()
        else:
            for q in range(1, nt):
                wt_in(j, lax.rem(t + q, nt)).wait_recv()
        sp[j] = jnp.dot(x_ref[...], wf[j], preferred_element_type=F32)
        swap = rc(sp.at[j, theirs], spx.at[j], px_s.at[j], px_r.at[j], partner)
        swap.start()
        swap.wait_recv()
        ssum[j] = sp[j, mine, :] + spx[j]

    def rs(side, j):
        return rc(ssum.at[j], srr.at[side, j], rs_s.at[j], rs_r.at[side, j],
                  {"voc": z + (1 if side else -1)})

    def student_step(d):
        for side, (j, ok) in enumerate(sides(d)):
            @pl.when(ok)
            def _(j=j, side=side):
                student(j, False)

                @pl.when(room[1 - side])
                def _():
                    rs(side, j).wait_recv()
                    ssum[j] += srr[side, j]
                rs(side, j).start()

    take_y(1, False)
    student_step(n - 1)
    dot_y(1)
    for d in range(n - 2, 0, -1):
        if d == 1:
            for e in range(2, n - 1):
                take_y(e, True)
        student_step(d)
    student(z, True)
    for side in range(2):
        @pl.when(room[1 - side])
        def _(side=side):
            rs(side, z).wait_recv()
            ssum[z] += srr[side, z]
    sl = ssum[z]
    ms = jnp.max(sl, axis=1, keepdims=True)
    ss = jnp.sum(jnp.exp(sl - ms), axis=1, keepdims=True)
    take_y(n - 1, True)

    tx = rc(tacc.at[theirs], tpx, px_s.at[n], px_r.at[n], partner)
    tx.start()
    tx.wait_recv()
    tl = tacc[mine, :] + tpx[...]
    tpx[...] = tl
    mt = jnp.max(tl, axis=1, keepdims=True)
    et = jnp.exp(tl - mt)
    st = jnp.sum(et, axis=1, keepdims=True)
    cr = jnp.sum(et * (tl - sl), axis=1, keepdims=True)
    lane = lax.broadcasted_iota(jnp.int32, (half, 128), 1)
    stat[z] = jnp.where(lane == 0, ms, jnp.where(lane == 1, mt, jnp.where(
        lane == 2, ss, jnp.where(lane == 3, st, cr))))

    def stx(j, src):
        return rc(stat.at[src], stat.at[src], st_s.at[j], st_r.at[src], {"voc": j})

    for k in range(1, n):
        stx(zdev(k), z).start()
    for k in range(1, n):
        stx(zdev(k), zdev(k)).wait_recv()
    parts = [stat[j] for j in range(n)]
    top = parts[0]
    for p in parts[1:]:
        top = jnp.maximum(top, p)
    big_s, big_t = top[:, 0:1], top[:, 1:2]
    tot_s = jnp.zeros_like(big_s)
    tot_t = jnp.zeros_like(big_s)
    cross = jnp.zeros_like(big_s)
    for p in parts:
        es = jnp.exp(p[:, 0:1] - big_s)
        ets = jnp.exp(p[:, 1:2] - big_t)
        tot_s = tot_s + p[:, 2:3] * es
        tot_t = tot_t + p[:, 3:4] * ets
        cross = cross + p[:, 4:5] * ets
    lse_s = big_s + jnp.log(tot_s)
    lse_t = big_t + jnp.log(tot_t)
    scale = wcol[mine, :][:, 0:1]
    gap[z, mine, :] = (scale * (jnp.exp(ssum[z] - lse_s) - jnp.exp(tpx[...] - lse_t))).astype(BF16)

    def gz(j, src):
        return rc(gap.at[src, mine], gap.at[src, mine], gz_s.at[j], gz_r.at[src], {"voc": j})

    def gx(src, side):
        return rc(gap.at[src, side], gap.at[src, side], gx_s.at[src], gx_r.at[src], partner)

    for d in range(1, n):
        for j, ok in sides(d):
            @pl.when(ok)
            def _(j=j):
                gz(j, z).start()
    gx(z, mine).start()

    div = cross / tot_t - lse_t + lse_s
    lossb[me] = jnp.broadcast_to(jnp.sum(div, axis=0, keepdims=True), (8, 128))

    def ls(a, b, src):
        return rc(lossb.at[src], lossb.at[src], ls_s.at[a * 2 + b], ls_r.at[src], {"tok": a, "hid": b})

    for (a, b) in plane:
        ls(a, b, me).start()

    def grad_dot(j, first):
        term = lax.dot_general(gap[j], wf[j], (((1,), (1,)), ((), ())), preferred_element_type=F32)
        if first:
            acc[...] = term
        else:
            acc[...] += term

    gx(z, theirs).wait_recv()
    grad_dot(z, True)
    for d in range(1, n):
        for j, ok in sides(d):
            @pl.when(ok)
            def _(j=j):
                gz(j, j).wait_recv()
                gx(j, mine).start()
    for k in range(1, n):
        j = zdev(k)
        gx(j, theirs).wait_recv()
        grad_dot(j, False)
    out[...] = acc[...].astype(BF16)

    for (a, b) in plane:
        ls(a, b, a * 2 + b).wait_recv()
    total = lossb[0]
    for p in range(1, nt * 2):
        total = total + lossb[p]
    loss_out[0, 0] = total[0, 0] / (rows * nt)

    for k in range(1, n):
        j = zdev(k)
        wz(j).wait_send()
        for q in range(1, nt):
            wt(j, lax.rem(t + q, nt)).wait_send()
        rc(ssum.at[j], srr.at[0, j], rs_s.at[j], rs_r.at[0, j], {"voc": j}).wait_send()
        stx(j, z).wait_send()
        gz(j, z).wait_send()
    for r in range(2):
        for side in range(2):
            @pl.when(room[side])
            def _(r=r, side=side):
                own_y(r, side).wait_send()
    for d in range(1, n - 1):
        for r in range(2):
            for side, (i, ok) in enumerate(sides(d)):
                on = 1 - side

                @pl.when(jnp.logical_and(ok, room[on]))
                def _(i=i, r=r, on=on):
                    relay_y(i, r, on).wait_send()
    for k in range(n):
        j = zdev(k)
        rc(sp.at[j, theirs], spx.at[j], px_s.at[j], px_r.at[j], partner).wait_send()
        gx(j, mine).wait_send()
    tx.wait_send()
    for (a, b) in plane:
        ls(a, b, me).wait_send()


def fused_shards(n, nt, student_hidden, teacher_hidden, student_head, teacher_head, loss_weight):
    rows, ks = student_hidden.shape
    kt = teacher_hidden.shape[1]
    v = student_head.shape[1]
    half = rows // 2
    dma = lambda *s: pltpu.SemaphoreType.DMA(s)
    vmem = lambda s, d: pltpu.VMEM(s, d)
    whole = pl.BlockSpec(memory_space=pltpu.VMEM)
    anywhere = pl.BlockSpec(memory_space=pl.ANY)
    grad, loss = pl.pallas_call(
        functools.partial(fused, n, nt),
        out_shape=(jax.ShapeDtypeStruct((rows, ks), BF16), jax.ShapeDtypeStruct((1, 1), F32)),
        in_specs=[anywhere] * 5,
        out_specs=(whole, pl.BlockSpec(memory_space=pltpu.SMEM)),
        scratch_shapes=[
            vmem((rows, ks), BF16),
            vmem((rows, kt), BF16),
            vmem((1, rows), F32),
            vmem((n, ks, v), BF16),
            vmem((n, kt, v), BF16),
            vmem((n, rows, kt), BF16),
            vmem((n, rows, v), F32),
            vmem((n, half, v), F32),
            vmem((n, half, v), F32),
            vmem((2, n, half, v), F32),
            vmem((rows, v), F32),
            vmem((half, v), F32),
            vmem((n, half, 128), F32),
            vmem((n, rows, v), BF16),
            vmem((rows, rows), F32),
            vmem((nt * 2, 8, 128), F32),
            vmem((rows, ks), F32),
            dma(n + 4),
            dma(n), dma(n), dma(n, nt), dma(n, nt),
            dma(2, n, 2), dma(n, 2),
            dma(n + 1), dma(n + 1), dma(n), dma(2, n),
            dma(n), dma(n), dma(n), dma(n), dma(n), dma(n),
            dma(nt * 2), dma(nt * 2),
        ],
        compiler_params=pltpu.CompilerParams(
            collective_id=0, has_side_effects=True, vmem_limit_bytes=48 << 20),
        name="divergence_grad",
    )(student_hidden, teacher_hidden, loss_weight.reshape(1, rows), student_head, teacher_head)
    return grad, loss.reshape(())


def divergence_terms(student_logits, teacher_logits, weights):
    differences = teacher_logits - student_logits
    peak_student, peak_teacher = lax.pmax(
        (jnp.max(student_logits, axis=1), jnp.max(teacher_logits, axis=1)), "voc"
    )
    scaled_student = jnp.exp(student_logits - peak_student[:, None])
    scaled_teacher = jnp.exp(teacher_logits - peak_teacher[:, None])
    total_student, total_teacher, cross_sum = lax.psum(
        (
            jnp.sum(scaled_student, axis=1),
            jnp.sum(scaled_teacher, axis=1),
            jnp.sum(scaled_teacher * differences, axis=1),
        ),
        "voc",
    )
    student_lse = peak_student + jnp.log(total_student)
    teacher_lse = peak_teacher + jnp.log(total_teacher)
    divergence = cross_sum / total_teacher - teacher_lse + student_lse
    prob_gap = jnp.exp(student_logits - student_lse[:, None]) - jnp.exp(
        teacher_logits - teacher_lse[:, None]
    )
    scaled_gap = (weights[:, None] * prob_gap).astype(jnp.bfloat16)
    return (divergence, scaled_gap)


def plain_shards(student_hidden, teacher_hidden, student_head, teacher_head, loss_weight):
    student_block, teacher_block = (
        lax.all_gather(student_hidden, "voc", axis=1, tiled=True),
        lax.all_gather(teacher_hidden, "voc", axis=1, tiled=True),
    )
    vocab_local = student_head.shape[1]
    row_count = student_block.shape[0] // lax.axis_size("hid")
    joined = lax.psum_scatter(
        jnp.concatenate(
            [
                jnp.dot(student_block, student_head, preferred_element_type=jnp.float32),
                jnp.dot(teacher_block, teacher_head, preferred_element_type=jnp.float32),
            ],
            axis=1,
        ),
        "hid",
        scatter_dimension=0,
        tiled=True,
    )
    student_logits = joined[:, :vocab_local]
    teacher_logits = joined[:, vocab_local:]
    weights = lax.dynamic_slice_in_dim(loss_weight, lax.axis_index("hid") * row_count, row_count)
    divergence, scaled_gap = divergence_terms(student_logits, teacher_logits, weights)
    token_total = loss_weight.shape[0] * lax.axis_size("tok")
    loss_total = lax.psum(jnp.sum(divergence), ("tok", "hid"))
    grad_terms = lax.dot_general(
        lax.all_gather(scaled_gap, "hid", axis=0, tiled=True),
        student_head,
        (((1,), (1,)), ((), ())),
        preferred_element_type=jnp.float32,
    )
    grad_hidden = lax.psum_scatter(grad_terms, "voc", scatter_dimension=1, tiled=True).astype(
        jnp.bfloat16
    )
    mean_loss = loss_total / token_total
    return (grad_hidden, mean_loss)


def solution(mesh):
    placed = (
        P("tok", ("hid", "voc")),
        P("tok", ("hid", "voc")),
        P("hid", "voc"),
        P("hid", "voc"),
        P("tok"),
    )
    n, nt = mesh.shape["voc"], mesh.shape["tok"]
    if 2 < n <= 4 and mesh.shape["hid"] == 2:
        body = functools.partial(fused_shards, n, nt)
    else:
        body = plain_shards
    return jax.shard_map(
        body,
        mesh=mesh,
        in_specs=placed,
        out_specs=(P("tok", ("hid", "voc")), P()),
        check_vma=False,
    )
```

```python
import functools

import jax
import jax.numpy as jnp
from jax import lax
from jax.experimental import pallas as pl
from jax.experimental.pallas import tpu as pltpu
from jax.sharding import PartitionSpec as P

MESH = pl.DeviceIdType.MESH
F32 = jnp.float32
BF16 = jnp.bfloat16


def fused(n, nt, x_hbm, y_hbm, w_hbm, sw_hbm, tw_hbm, out, loss_out,
          x_ref, y_ref, w_ref, wf, tw, tg, sp, spx, ssum, srr, tacc, tpx, stat, gap, wcol, lossb, acc,
          lc, wz_s, wz_r, wt_s, wt_r, th_s, th_r, px_s, px_r, rs_s, rs_r,
          st_s, st_r, gz_s, gz_r, gx_s, gx_r, ls_s, ls_r):
    z = lax.axis_index("voc")
    t = lax.axis_index("tok")
    h = lax.axis_index("hid")
    rows, ks = x_ref.shape
    kt = y_ref.shape[1]
    half = rows // 2
    quarter = ks // nt
    partner = {"hid": 1 - h}
    mine = pl.ds(pl.multiple_of(h * half, half), half)
    theirs = pl.ds(pl.multiple_of((1 - h) * half, half), half)
    me = t * 2 + h

    def rc(src, dst, ss, rs, dev):
        return pltpu.make_async_remote_copy(
            src_ref=src, dst_ref=dst, send_sem=ss, recv_sem=rs,
            device_id=dev, device_id_type=MESH)

    def zdev(k):
        return lax.rem(z + k, n)

    plane = []
    for q in range(nt):
        for c in range(2):
            if q or c:
                plane.append((lax.rem(t + q, nt), lax.rem(h + c, 2)))

    own_w = pltpu.make_async_copy(sw_hbm.at[pl.ds(pl.multiple_of(z * ks, ks), ks)], wf.at[z], lc.at[n])
    own_w.start()
    ins = [pltpu.make_async_copy(a, b, lc.at[n + 1 + i])
           for i, (a, b) in enumerate(((x_hbm, x_ref), (y_hbm, y_ref), (w_hbm, w_ref)))]
    for c in ins:
        c.start()

    def tw_copy(i):
        return pltpu.make_async_copy(tw_hbm.at[pl.ds(pl.multiple_of(i * kt, kt), kt)], tw.at[i], lc.at[i])

    barrier = pltpu.get_barrier_semaphore()
    for k in range(1, n):
        pl.semaphore_signal(barrier, inc=1, device_id={"voc": zdev(k)}, device_id_type=MESH)
    for (a, b) in plane:
        pl.semaphore_signal(barrier, inc=1, device_id={"tok": a, "hid": b}, device_id_type=MESH)
    pl.semaphore_wait(barrier, n - 1 + len(plane))

    def part(i):
        return pl.ds(pl.multiple_of(i * quarter, quarter), quarter)

    def wz(j):
        return rc(sw_hbm.at[pl.ds(pl.multiple_of(j * ks + t * quarter, quarter), quarter)],
                  wf.at[z, part(t)], wz_s.at[j], wz_r.at[z], {"voc": j})

    def wz_in(j):
        return rc(wf.at[j, part(t)], wf.at[j, part(t)], wz_s.at[j], wz_r.at[j], {"voc": j})

    def wt(j, dst_t):
        return rc(wf.at[j, part(t)], wf.at[j, part(t)], wt_s.at[j, dst_t], wt_r.at[j, t], {"tok": dst_t})

    def wt_in(j, src_t):
        return rc(wf.at[j, part(src_t)], wf.at[j, part(src_t)], wt_s.at[j, src_t], wt_r.at[j, src_t], {"tok": src_t})

    def sides(d):
        return ((z - d, z - d >= 0), (z + d, z + d < n))

    for d in range(n - 1, 0, -1):
        for j, ok in sides(d):
            @pl.when(ok)
            def _(j=j):
                wz(j).start()

    def piece(r):
        return pl.ds(r * half, half)

    def own_y(r, side):
        return rc(y_hbm.at[piece(r)], tg.at[z, piece(r)], th_s.at[side, z, r], th_r.at[z, r],
                  {"voc": z + (1 if side else -1)})

    def relay_y(i, r, side):
        return rc(tg.at[i, piece(r)], tg.at[i, piece(r)], th_s.at[side, i, r], th_r.at[i, r],
                  {"voc": z + (1 if side else -1)})

    room = (z - 1 >= 0, z + 1 < n)
    for r in range(2):
        for side in range(2):
            @pl.when(room[side])
            def _(r=r, side=side):
                own_y(r, side).start()

    for k in range(n):
        tw_copy(zdev(k)).start()

    for c in ins:
        c.wait()
    wcol[...] = jnp.transpose(jnp.broadcast_to(w_ref[...], (rows, rows)))

    for d in range(n - 1, 0, -1):
        for j, ok in sides(d):
            @pl.when(ok)
            def _(j=j):
                wz_in(j).wait_recv()
                for q in range(1, nt):
                    wt(j, lax.rem(t + q, nt)).start()

    def teacher_dot(src, i, first):
        tw_copy(i).wait()
        step = kt // 2

        @pl.loop(0, 2)
        def _(s):
            cols = pl.ds(pl.multiple_of(s * step, step), step)
            term = jnp.dot(src[:, cols], tw[i, cols, :], preferred_element_type=F32)
            if first:
                @pl.when(s == 0)
                def _():
                    tacc[...] = term

                @pl.when(s > 0)
                def _():
                    tacc[...] += term
            else:
                tacc[...] += term

    teacher_dot(y_ref, z, True)

    def take_y(d, dot):
        for r in range(2):
            for side, (i, ok) in enumerate(sides(d)):
                @pl.when(ok)
                def _(i=i, side=side, r=r):
                    relay_y(i, r, side).wait_recv()
                    if d < n - 1:
                        on = 1 - side

                        @pl.when(room[on])
                        def _():
                            relay_y(i, r, on).start()
        if dot:
            dot_y(d)

    def dot_y(d):
        for i, ok in sides(d):
            @pl.when(ok)
            def _(i=i):
                teacher_dot(tg.at[i], i, False)

    def student(j, own):
        if own:
            own_w.wait()
        else:
            for q in range(1, nt):
                wt_in(j, lax.rem(t + q, nt)).wait_recv()
        sp[j] = jnp.dot(x_ref[...], wf[j], preferred_element_type=F32)
        swap = rc(sp.at[j, theirs], spx.at[j], px_s.at[j], px_r.at[j], partner)
        swap.start()
        swap.wait_recv()
        ssum[j] = sp[j, mine, :] + spx[j]

    def rs(side, j):
        return rc(ssum.at[j], srr.at[side, j], rs_s.at[j], rs_r.at[side, j],
                  {"voc": z + (1 if side else -1)})

    def student_step(d):
        for side, (j, ok) in enumerate(sides(d)):
            @pl.when(ok)
            def _(j=j, side=side):
                student(j, False)

                @pl.when(room[1 - side])
                def _():
                    rs(side, j).wait_recv()
                    ssum[j] += srr[side, j]
                rs(side, j).start()

    take_y(1, False)
    student_step(n - 1)
    dot_y(1)
    for d in range(n - 2, 0, -1):
        if d == 1:
            for e in range(2, n - 1):
                take_y(e, True)
        student_step(d)
    student(z, True)
    for side in range(2):
        @pl.when(room[1 - side])
        def _(side=side):
            rs(side, z).wait_recv()
            ssum[z] += srr[side, z]
    sl = ssum[z]
    ms = jnp.max(sl, axis=1, keepdims=True)
    ss = jnp.sum(jnp.exp(sl - ms), axis=1, keepdims=True)
    take_y(n - 1, True)

    tx = rc(tacc.at[theirs], tpx, px_s.at[n], px_r.at[n], partner)
    tx.start()
    tx.wait_recv()
    tl = tacc[mine, :] + tpx[...]
    tpx[...] = tl
    mt = jnp.max(tl, axis=1, keepdims=True)
    et = jnp.exp(tl - mt)
    st = jnp.sum(et, axis=1, keepdims=True)
    cr = jnp.sum(et * (tl - sl), axis=1, keepdims=True)
    lane = lax.broadcasted_iota(jnp.int32, (half, 128), 1)
    stat[z] = jnp.where(lane == 0, ms, jnp.where(lane == 1, mt, jnp.where(
        lane == 2, ss, jnp.where(lane == 3, st, cr))))

    def stx(j, src):
        return rc(stat.at[src], stat.at[src], st_s.at[j], st_r.at[src], {"voc": j})

    for k in range(1, n):
        stx(zdev(k), z).start()
    for k in range(1, n):
        stx(zdev(k), zdev(k)).wait_recv()
    parts = [stat[j] for j in range(n)]
    top = parts[0]
    for p in parts[1:]:
        top = jnp.maximum(top, p)
    big_s, big_t = top[:, 0:1], top[:, 1:2]
    tot_s = jnp.zeros_like(big_s)
    tot_t = jnp.zeros_like(big_s)
    cross = jnp.zeros_like(big_s)
    for p in parts:
        es = jnp.exp(p[:, 0:1] - big_s)
        ets = jnp.exp(p[:, 1:2] - big_t)
        tot_s = tot_s + p[:, 2:3] * es
        tot_t = tot_t + p[:, 3:4] * ets
        cross = cross + p[:, 4:5] * ets
    lse_s = big_s + jnp.log(tot_s)
    lse_t = big_t + jnp.log(tot_t)
    scale = wcol[mine, :][:, 0:1]
    gap[z, mine, :] = (scale * (jnp.exp(ssum[z] - lse_s) - jnp.exp(tpx[...] - lse_t))).astype(BF16)

    def gz(j, src):
        return rc(gap.at[src, mine], gap.at[src, mine], gz_s.at[j], gz_r.at[src], {"voc": j})

    def gx(src, side):
        return rc(gap.at[src, side], gap.at[src, side], gx_s.at[src], gx_r.at[src], partner)

    for d in range(1, n):
        for j, ok in sides(d):
            @pl.when(ok)
            def _(j=j):
                gz(j, z).start()
    gx(z, mine).start()

    div = cross / tot_t - lse_t + lse_s
    lossb[me] = jnp.broadcast_to(jnp.sum(div, axis=0, keepdims=True), (8, 128))

    def ls(a, b, src):
        return rc(lossb.at[src], lossb.at[src], ls_s.at[a * 2 + b], ls_r.at[src], {"tok": a, "hid": b})

    for (a, b) in plane:
        ls(a, b, me).start()

    def grad_dot(j, first):
        term = lax.dot_general(gap[j], wf[j], (((1,), (1,)), ((), ())), preferred_element_type=F32)
        if first:
            acc[...] = term
        else:
            acc[...] += term

    gx(z, theirs).wait_recv()
    grad_dot(z, True)
    for d in range(1, n):
        for j, ok in sides(d):
            @pl.when(ok)
            def _(j=j):
                gz(j, j).wait_recv()
                gx(j, mine).start()
    for k in range(1, n):
        j = zdev(k)
        gx(j, theirs).wait_recv()
        grad_dot(j, False)
    out[...] = acc[...].astype(BF16)

    for (a, b) in plane:
        ls(a, b, a * 2 + b).wait_recv()
    total = lossb[0]
    for p in range(1, nt * 2):
        total = total + lossb[p]
    loss_out[0, 0] = total[0, 0] / (rows * nt)

    for k in range(1, n):
        j = zdev(k)
        wz(j).wait_send()
        for q in range(1, nt):
            wt(j, lax.rem(t + q, nt)).wait_send()
        rc(ssum.at[j], srr.at[0, j], rs_s.at[j], rs_r.at[0, j], {"voc": j}).wait_send()
        stx(j, z).wait_send()
        gz(j, z).wait_send()
    for r in range(2):
        for side in range(2):
            @pl.when(room[side])
            def _(r=r, side=side):
                own_y(r, side).wait_send()
    for d in range(1, n - 1):
        for r in range(2):
            for side, (i, ok) in enumerate(sides(d)):
                on = 1 - side

                @pl.when(jnp.logical_and(ok, room[on]))
                def _(i=i, r=r, on=on):
                    relay_y(i, r, on).wait_send()
    for k in range(n):
        j = zdev(k)
        rc(sp.at[j, theirs], spx.at[j], px_s.at[j], px_r.at[j], partner).wait_send()
        gx(j, mine).wait_send()
    tx.wait_send()
    for (a, b) in plane:
        ls(a, b, me).wait_send()


def fused_shards(n, nt, student_hidden, teacher_hidden, student_head, teacher_head, loss_weight):
    rows, ks = student_hidden.shape
    kt = teacher_hidden.shape[1]
    v = student_head.shape[1]
    half = rows // 2
    dma = lambda *s: pltpu.SemaphoreType.DMA(s)
    vmem = lambda s, d: pltpu.VMEM(s, d)
    whole = pl.BlockSpec(memory_space=pltpu.VMEM)
    anywhere = pl.BlockSpec(memory_space=pl.ANY)
    grad, loss = pl.pallas_call(
        functools.partial(fused, n, nt),
        out_shape=(jax.ShapeDtypeStruct((rows, ks), BF16), jax.ShapeDtypeStruct((1, 1), F32)),
        in_specs=[anywhere] * 5,
        out_specs=(whole, pl.BlockSpec(memory_space=pltpu.SMEM)),
        scratch_shapes=[
            vmem((rows, ks), BF16),
            vmem((rows, kt), BF16),
            vmem((1, rows), F32),
            vmem((n, ks, v), BF16),
            vmem((n, kt, v), BF16),
            vmem((n, rows, kt), BF16),
            vmem((n, rows, v), F32),
            vmem((n, half, v), F32),
            vmem((n, half, v), F32),
            vmem((2, n, half, v), F32),
            vmem((rows, v), F32),
            vmem((half, v), F32),
            vmem((n, half, 128), F32),
            vmem((n, rows, v), BF16),
            vmem((rows, rows), F32),
            vmem((nt * 2, 8, 128), F32),
            vmem((rows, ks), F32),
            dma(n + 4),
            dma(n), dma(n), dma(n, nt), dma(n, nt),
            dma(2, n, 2), dma(n, 2),
            dma(n + 1), dma(n + 1), dma(n), dma(2, n),
            dma(n), dma(n), dma(n), dma(n), dma(n), dma(n),
            dma(nt * 2), dma(nt * 2),
        ],
        compiler_params=pltpu.CompilerParams(
            collective_id=0, has_side_effects=True, vmem_limit_bytes=60 << 20),
        name="divergence_grad",
    )(student_hidden, teacher_hidden, loss_weight.reshape(1, rows), student_head, teacher_head)
    return grad, loss.reshape(())


def divergence_terms(student_logits, teacher_logits, weights):
    differences = teacher_logits - student_logits
    peak_student, peak_teacher = lax.pmax(
        (jnp.max(student_logits, axis=1), jnp.max(teacher_logits, axis=1)), "voc"
    )
    scaled_student = jnp.exp(student_logits - peak_student[:, None])
    scaled_teacher = jnp.exp(teacher_logits - peak_teacher[:, None])
    total_student, total_teacher, cross_sum = lax.psum(
        (
            jnp.sum(scaled_student, axis=1),
            jnp.sum(scaled_teacher, axis=1),
            jnp.sum(scaled_teacher * differences, axis=1),
        ),
        "voc",
    )
    student_lse = peak_student + jnp.log(total_student)
    teacher_lse = peak_teacher + jnp.log(total_teacher)
    divergence = cross_sum / total_teacher - teacher_lse + student_lse
    prob_gap = jnp.exp(student_logits - student_lse[:, None]) - jnp.exp(
        teacher_logits - teacher_lse[:, None]
    )
    scaled_gap = (weights[:, None] * prob_gap).astype(jnp.bfloat16)
    return (divergence, scaled_gap)


def plain_shards(student_hidden, teacher_hidden, student_head, teacher_head, loss_weight):
    student_block, teacher_block = (
        lax.all_gather(student_hidden, "voc", axis=1, tiled=True),
        lax.all_gather(teacher_hidden, "voc", axis=1, tiled=True),
    )
    vocab_local = student_head.shape[1]
    row_count = student_block.shape[0] // lax.axis_size("hid")
    joined = lax.psum_scatter(
        jnp.concatenate(
            [
                jnp.dot(student_block, student_head, preferred_element_type=jnp.float32),
                jnp.dot(teacher_block, teacher_head, preferred_element_type=jnp.float32),
            ],
            axis=1,
        ),
        "hid",
        scatter_dimension=0,
        tiled=True,
    )
    student_logits = joined[:, :vocab_local]
    teacher_logits = joined[:, vocab_local:]
    weights = lax.dynamic_slice_in_dim(loss_weight, lax.axis_index("hid") * row_count, row_count)
    divergence, scaled_gap = divergence_terms(student_logits, teacher_logits, weights)
    token_total = loss_weight.shape[0] * lax.axis_size("tok")
    loss_total = lax.psum(jnp.sum(divergence), ("tok", "hid"))
    grad_terms = lax.dot_general(
        lax.all_gather(scaled_gap, "hid", axis=0, tiled=True),
        student_head,
        (((1,), (1,)), ((), ())),
        preferred_element_type=jnp.float32,
    )
    grad_hidden = lax.psum_scatter(grad_terms, "voc", scatter_dimension=1, tiled=True).astype(
        jnp.bfloat16
    )
    mean_loss = loss_total / token_total
    return (grad_hidden, mean_loss)


def solution(mesh):
    placed = (
        P("tok", ("hid", "voc")),
        P("tok", ("hid", "voc")),
        P("hid", "voc"),
        P("hid", "voc"),
        P("tok"),
    )
    n, nt = mesh.shape["voc"], mesh.shape["tok"]
    if 2 < n <= 4 and mesh.shape["hid"] == 2:
        body = functools.partial(fused_shards, n, nt)
    else:
        body = plain_shards
    return jax.shard_map(
        body,
        mesh=mesh,
        in_specs=placed,
        out_specs=(P("tok", ("hid", "voc")), P()),
        check_vma=False,
    )
```

```python
import functools

import jax
import jax.numpy as jnp
from jax import lax
from jax.experimental import pallas as pl
from jax.experimental.pallas import tpu as pltpu
from jax.sharding import PartitionSpec as P

MESH = pl.DeviceIdType.MESH
F32 = jnp.float32
BF16 = jnp.bfloat16


def fused(n, nt, x_hbm, y_hbm, w_hbm, sw_hbm, tw_hbm, out, loss_out,
          x_ref, y_ref, w_ref, wf, tw, tg, sp, spx, ssum, srr, tacc, tpx, stat, gap, wcol, lossb, acc,
          lc, wz_s, wz_r, wt_s, wt_r, th_s, th_r, px_s, px_r, rs_s, rs_r,
          st_s, st_r, gz_s, gz_r, gx_s, gx_r, ls_s, ls_r):
    z = lax.axis_index("voc")
    t = lax.axis_index("tok")
    h = lax.axis_index("hid")
    rows, ks = x_ref.shape
    kt = y_ref.shape[1]
    half = rows // 2
    quarter = ks // nt
    partner = {"hid": 1 - h}
    mine = pl.ds(pl.multiple_of(h * half, half), half)
    theirs = pl.ds(pl.multiple_of((1 - h) * half, half), half)
    me = t * 2 + h

    def rc(src, dst, ss, rs, dev):
        return pltpu.make_async_remote_copy(
            src_ref=src, dst_ref=dst, send_sem=ss, recv_sem=rs,
            device_id=dev, device_id_type=MESH)

    def zdev(k):
        return lax.rem(z + k, n)

    plane = []
    for q in range(nt):
        for c in range(2):
            if q or c:
                plane.append((lax.rem(t + q, nt), lax.rem(h + c, 2)))

    own_w = pltpu.make_async_copy(sw_hbm.at[pl.ds(pl.multiple_of(z * ks, ks), ks)], wf.at[z], lc.at[n])
    own_w.start()
    ins = [pltpu.make_async_copy(a, b, lc.at[n + 1 + i])
           for i, (a, b) in enumerate(((x_hbm, x_ref), (y_hbm, y_ref), (w_hbm, w_ref)))]
    for c in ins:
        c.start()

    def tw_copy(i):
        return pltpu.make_async_copy(tw_hbm.at[pl.ds(pl.multiple_of(i * kt, kt), kt)], tw.at[i], lc.at[i])

    barrier = pltpu.get_barrier_semaphore()
    for k in range(1, n):
        pl.semaphore_signal(barrier, inc=1, device_id={"voc": zdev(k)}, device_id_type=MESH)
    for (a, b) in plane:
        pl.semaphore_signal(barrier, inc=1, device_id={"tok": a, "hid": b}, device_id_type=MESH)
    pl.semaphore_wait(barrier, n - 1 + len(plane))

    def part(i):
        return pl.ds(pl.multiple_of(i * quarter, quarter), quarter)

    def wz(j):
        return rc(sw_hbm.at[pl.ds(pl.multiple_of(j * ks + t * quarter, quarter), quarter)],
                  wf.at[z, part(t)], wz_s.at[j], wz_r.at[z], {"voc": j})

    def wz_in(j):
        return rc(wf.at[j, part(t)], wf.at[j, part(t)], wz_s.at[j], wz_r.at[j], {"voc": j})

    side_x = t + 1 - 2 * lax.rem(t, 2)
    side_y = lax.rem(t + 2, 4)
    opposite = 3 - t
    near = (side_x, side_y)

    def wt(j, o, p, to):
        rows_of = pl.ds(pl.multiple_of(o * quarter + p * (quarter // 2), quarter // 2), quarter // 2)
        return rc(wf.at[j, rows_of], wf.at[j, rows_of], wt_s.at[to, j, o, p], wt_r.at[j, o, p],
                  {"tok": near[to]})

    def spread(j):
        for i in range(2):
            wt(j, t, i, 0).start()
            wt(j, t, 1 - i, 1).start()

    def pass_on(j):
        for p in range(2):
            wt(j, near[p], p, 1 - p).wait_recv()
            wt(j, near[p], p, 1 - p).start()

    def sides(d):
        return ((z - d, z - d >= 0), (z + d, z + d < n))

    for d in range(n - 1, 0, -1):
        for j, ok in sides(d):
            @pl.when(ok)
            def _(j=j):
                wz(j).start()

    def piece(r):
        return pl.ds(r * half, half)

    def own_y(r, side):
        return rc(y_hbm.at[piece(r)], tg.at[z, piece(r)], th_s.at[side, z, r], th_r.at[z, r],
                  {"voc": z + (1 if side else -1)})

    def relay_y(i, r, side):
        return rc(tg.at[i, piece(r)], tg.at[i, piece(r)], th_s.at[side, i, r], th_r.at[i, r],
                  {"voc": z + (1 if side else -1)})

    room = (z - 1 >= 0, z + 1 < n)
    for r in range(2):
        for side in range(2):
            @pl.when(room[side])
            def _(r=r, side=side):
                own_y(r, side).start()

    for k in range(n):
        tw_copy(zdev(k)).start()

    for c in ins:
        c.wait()
    wcol[...] = jnp.transpose(jnp.broadcast_to(w_ref[...], (rows, rows)))

    for d in range(n - 1, 0, -1):
        for j, ok in sides(d):
            @pl.when(ok)
            def _(j=j):
                wz_in(j).wait_recv()
                spread(j)

    def teacher_dot(src, i, first):
        tw_copy(i).wait()
        step = kt // 2

        @pl.loop(0, 2)
        def _(s):
            cols = pl.ds(pl.multiple_of(s * step, step), step)
            term = jnp.dot(src[:, cols], tw[i, cols, :], preferred_element_type=F32)
            if first:
                @pl.when(s == 0)
                def _():
                    tacc[...] = term

                @pl.when(s > 0)
                def _():
                    tacc[...] += term
            else:
                tacc[...] += term

    teacher_dot(y_ref, z, True)

    def take_y(d, dot):
        for r in range(2):
            for side, (i, ok) in enumerate(sides(d)):
                @pl.when(ok)
                def _(i=i, side=side, r=r):
                    relay_y(i, r, side).wait_recv()
                    if d < n - 1:
                        on = 1 - side

                        @pl.when(room[on])
                        def _():
                            relay_y(i, r, on).start()
        if dot:
            dot_y(d)

    def dot_y(d):
        for i, ok in sides(d):
            @pl.when(ok)
            def _(i=i):
                teacher_dot(tg.at[i], i, False)

    def student(j, own):
        if own:
            own_w.wait()
        else:
            wt(j, side_x, 1, 0).wait_recv()
            wt(j, side_y, 0, 0).wait_recv()
            wt(j, opposite, 0, 0).wait_recv()
            wt(j, opposite, 1, 0).wait_recv()
        sp[j] = jnp.dot(x_ref[...], wf[j], preferred_element_type=F32)
        swap = rc(sp.at[j, theirs], spx.at[j], px_s.at[j], px_r.at[j], partner)
        swap.start()
        swap.wait_recv()
        ssum[j] = sp[j, mine, :] + spx[j]

    def rs(side, j):
        return rc(ssum.at[j], srr.at[side, j], rs_s.at[j], rs_r.at[side, j],
                  {"voc": z + (1 if side else -1)})

    def student_step(d):
        for side, (j, ok) in enumerate(sides(d)):
            @pl.when(ok)
            def _(j=j, side=side):
                student(j, False)

                @pl.when(room[1 - side])
                def _():
                    rs(side, j).wait_recv()
                    ssum[j] += srr[side, j]
                rs(side, j).start()

    take_y(1, False)
    for d in range(n - 1, 0, -1):
        for j, ok in sides(d):
            @pl.when(ok)
            def _(j=j):
                pass_on(j)
    student_step(n - 1)
    dot_y(1)
    for d in range(n - 2, 0, -1):
        if d == 1:
            for e in range(2, n - 1):
                take_y(e, True)
        student_step(d)
    student(z, True)
    for side in range(2):
        @pl.when(room[1 - side])
        def _(side=side):
            rs(side, z).wait_recv()
            ssum[z] += srr[side, z]
    sl = ssum[z]
    ms = jnp.max(sl, axis=1, keepdims=True)
    ss = jnp.sum(jnp.exp(sl - ms), axis=1, keepdims=True)
    take_y(n - 1, True)

    tx = rc(tacc.at[theirs], tpx, px_s.at[n], px_r.at[n], partner)
    tx.start()
    tx.wait_recv()
    tl = tacc[mine, :] + tpx[...]
    tpx[...] = tl
    mt = jnp.max(tl, axis=1, keepdims=True)
    et = jnp.exp(tl - mt)
    st = jnp.sum(et, axis=1, keepdims=True)
    cr = jnp.sum(et * (tl - sl), axis=1, keepdims=True)
    lane = lax.broadcasted_iota(jnp.int32, (half, 128), 1)
    cols = jnp.where(lane == 0, ms, jnp.where(lane == 1, mt, jnp.where(
        lane == 2, ss, jnp.where(lane == 3, st, cr))))
    stat[z] = jnp.transpose(jnp.concatenate([cols] * (128 // half), axis=0))[:8]

    def stx(j, src):
        return rc(stat.at[src], stat.at[src], st_s.at[j], st_r.at[src], {"voc": j})

    for k in range(1, n):
        stx(zdev(k), z).start()
    for k in range(1, n):
        stx(zdev(k), zdev(k)).wait_recv()
    parts = [stat[j] for j in range(n)]
    top = parts[0]
    for p in parts[1:]:
        top = jnp.maximum(top, p)
    big_s, big_t = top[0:1], top[1:2]
    tot_s = jnp.zeros_like(big_s)
    tot_t = jnp.zeros_like(big_s)
    cross = jnp.zeros_like(big_s)
    for p in parts:
        es = jnp.exp(p[0:1] - big_s)
        ets = jnp.exp(p[1:2] - big_t)
        tot_s = tot_s + p[2:3] * es
        tot_t = tot_t + p[3:4] * ets
        cross = cross + p[4:5] * ets
    lse_s = big_s + jnp.log(tot_s)
    lse_t = big_t + jnp.log(tot_t)
    scale = wcol[mine, :][:, 0:1]
    sub = lax.broadcasted_iota(jnp.int32, (128, 128), 0)
    back = jnp.transpose(jnp.where(sub == 0, lse_s, lse_t))[:half]
    col_s, col_t = back[:, 0:1], back[:, 1:2]
    gap[z, mine, :] = (scale * (jnp.exp(ssum[z] - col_s) - jnp.exp(tpx[...] - col_t))).astype(BF16)

    def gz(j, src):
        return rc(gap.at[src, mine], gap.at[src, mine], gz_s.at[j], gz_r.at[src], {"voc": j})

    def gx(src, side):
        return rc(gap.at[src, side], gap.at[src, side], gx_s.at[src], gx_r.at[src], partner)

    for d in range(1, n):
        for j, ok in sides(d):
            @pl.when(ok)
            def _(j=j):
                gz(j, z).start()
    gx(z, mine).start()

    div = cross / tot_t - lse_t + lse_s
    first = lax.broadcasted_iota(jnp.int32, div.shape, 1) < half
    lossb[me] = jnp.broadcast_to(jnp.sum(jnp.where(first, div, 0.0), axis=1, keepdims=True), (8, 128))

    def ls(a, b, src):
        return rc(lossb.at[src], lossb.at[src], ls_s.at[a * 2 + b], ls_r.at[src], {"tok": a, "hid": b})

    for (a, b) in plane:
        ls(a, b, me).start()

    def grad_dot(j, first):
        term = lax.dot_general(gap[j], wf[j], (((1,), (1,)), ((), ())), preferred_element_type=F32)
        if first:
            acc[...] = term
        else:
            acc[...] += term

    gx(z, theirs).wait_recv()
    grad_dot(z, True)
    for d in range(1, n):
        for j, ok in sides(d):
            @pl.when(ok)
            def _(j=j):
                gz(j, j).wait_recv()
                gx(j, mine).start()
    for k in range(1, n):
        j = zdev(k)
        gx(j, theirs).wait_recv()
        grad_dot(j, False)
    out[...] = acc[...].astype(BF16)

    for (a, b) in plane:
        ls(a, b, a * 2 + b).wait_recv()
    total = lossb[0]
    for p in range(1, nt * 2):
        total = total + lossb[p]
    loss_out[0, 0] = total[0, 0] / (rows * nt)

    for k in range(1, n):
        j = zdev(k)
        wz(j).wait_send()
        for p in range(2):
            wt(j, t, p, 0).wait_send()
            wt(j, t, p, 1).wait_send()
            wt(j, near[p], p, 1 - p).wait_send()
        rc(ssum.at[j], srr.at[0, j], rs_s.at[j], rs_r.at[0, j], {"voc": j}).wait_send()
        stx(j, z).wait_send()
        gz(j, z).wait_send()
    for r in range(2):
        for side in range(2):
            @pl.when(room[side])
            def _(r=r, side=side):
                own_y(r, side).wait_send()
    for d in range(1, n - 1):
        for r in range(2):
            for side, (i, ok) in enumerate(sides(d)):
                on = 1 - side

                @pl.when(jnp.logical_and(ok, room[on]))
                def _(i=i, r=r, on=on):
                    relay_y(i, r, on).wait_send()
    for k in range(n):
        j = zdev(k)
        rc(sp.at[j, theirs], spx.at[j], px_s.at[j], px_r.at[j], partner).wait_send()
        gx(j, mine).wait_send()
    tx.wait_send()
    for (a, b) in plane:
        ls(a, b, me).wait_send()


def fused_shards(n, nt, student_hidden, teacher_hidden, student_head, teacher_head, loss_weight):
    rows, ks = student_hidden.shape
    kt = teacher_hidden.shape[1]
    v = student_head.shape[1]
    half = rows // 2
    dma = lambda *s: pltpu.SemaphoreType.DMA(s)
    vmem = lambda s, d: pltpu.VMEM(s, d)
    whole = pl.BlockSpec(memory_space=pltpu.VMEM)
    anywhere = pl.BlockSpec(memory_space=pl.ANY)
    grad, loss = pl.pallas_call(
        functools.partial(fused, n, nt),
        out_shape=(jax.ShapeDtypeStruct((rows, ks), BF16), jax.ShapeDtypeStruct((1, 1), F32)),
        in_specs=[anywhere] * 5,
        out_specs=(whole, pl.BlockSpec(memory_space=pltpu.SMEM)),
        scratch_shapes=[
            vmem((rows, ks), BF16),
            vmem((rows, kt), BF16),
            vmem((1, rows), F32),
            vmem((n, ks, v), BF16),
            vmem((n, kt, v), BF16),
            vmem((n, rows, kt), BF16),
            vmem((n, rows, v), F32),
            vmem((n, half, v), F32),
            vmem((n, half, v), F32),
            vmem((2, n, half, v), F32),
            vmem((rows, v), F32),
            vmem((half, v), F32),
            vmem((n, 8, 128), F32),
            vmem((n, rows, v), BF16),
            vmem((rows, rows), F32),
            vmem((nt * 2, 8, 128), F32),
            vmem((rows, ks), F32),
            dma(n + 4),
            dma(n), dma(n), dma(2, n, nt, 2), dma(n, nt, 2),
            dma(2, n, 2), dma(n, 2),
            dma(n + 1), dma(n + 1), dma(n), dma(2, n),
            dma(n), dma(n), dma(n), dma(n), dma(n), dma(n),
            dma(nt * 2), dma(nt * 2),
        ],
        compiler_params=pltpu.CompilerParams(
            collective_id=0, has_side_effects=True, vmem_limit_bytes=60 << 20),
        name="divergence_grad",
    )(student_hidden, teacher_hidden, loss_weight.reshape(1, rows), student_head, teacher_head)
    return grad, loss.reshape(())


def divergence_terms(student_logits, teacher_logits, weights):
    differences = teacher_logits - student_logits
    peak_student, peak_teacher = lax.pmax(
        (jnp.max(student_logits, axis=1), jnp.max(teacher_logits, axis=1)), "voc"
    )
    scaled_student = jnp.exp(student_logits - peak_student[:, None])
    scaled_teacher = jnp.exp(teacher_logits - peak_teacher[:, None])
    total_student, total_teacher, cross_sum = lax.psum(
        (
            jnp.sum(scaled_student, axis=1),
            jnp.sum(scaled_teacher, axis=1),
            jnp.sum(scaled_teacher * differences, axis=1),
        ),
        "voc",
    )
    student_lse = peak_student + jnp.log(total_student)
    teacher_lse = peak_teacher + jnp.log(total_teacher)
    divergence = cross_sum / total_teacher - teacher_lse + student_lse
    prob_gap = jnp.exp(student_logits - student_lse[:, None]) - jnp.exp(
        teacher_logits - teacher_lse[:, None]
    )
    scaled_gap = (weights[:, None] * prob_gap).astype(jnp.bfloat16)
    return (divergence, scaled_gap)


def plain_shards(student_hidden, teacher_hidden, student_head, teacher_head, loss_weight):
    student_block, teacher_block = (
        lax.all_gather(student_hidden, "voc", axis=1, tiled=True),
        lax.all_gather(teacher_hidden, "voc", axis=1, tiled=True),
    )
    vocab_local = student_head.shape[1]
    row_count = student_block.shape[0] // lax.axis_size("hid")
    joined = lax.psum_scatter(
        jnp.concatenate(
            [
                jnp.dot(student_block, student_head, preferred_element_type=jnp.float32),
                jnp.dot(teacher_block, teacher_head, preferred_element_type=jnp.float32),
            ],
            axis=1,
        ),
        "hid",
        scatter_dimension=0,
        tiled=True,
    )
    student_logits = joined[:, :vocab_local]
    teacher_logits = joined[:, vocab_local:]
    weights = lax.dynamic_slice_in_dim(loss_weight, lax.axis_index("hid") * row_count, row_count)
    divergence, scaled_gap = divergence_terms(student_logits, teacher_logits, weights)
    token_total = loss_weight.shape[0] * lax.axis_size("tok")
    loss_total = lax.psum(jnp.sum(divergence), ("tok", "hid"))
    grad_terms = lax.dot_general(
        lax.all_gather(scaled_gap, "hid", axis=0, tiled=True),
        student_head,
        (((1,), (1,)), ((), ())),
        preferred_element_type=jnp.float32,
    )
    grad_hidden = lax.psum_scatter(grad_terms, "voc", scatter_dimension=1, tiled=True).astype(
        jnp.bfloat16
    )
    mean_loss = loss_total / token_total
    return (grad_hidden, mean_loss)


def solution(mesh):
    placed = (
        P("tok", ("hid", "voc")),
        P("tok", ("hid", "voc")),
        P("hid", "voc"),
        P("hid", "voc"),
        P("tok"),
    )
    n, nt = mesh.shape["voc"], mesh.shape["tok"]
    if 2 < n <= 4 and nt == 4 and mesh.shape["hid"] == 2:
        body = functools.partial(fused_shards, n, nt)
    else:
        body = plain_shards
    return jax.shard_map(
        body,
        mesh=mesh,
        in_specs=placed,
        out_specs=(P("tok", ("hid", "voc")), P()),
        check_vma=False,
    )
```

```python
import functools

import jax
import jax.numpy as jnp
from jax import lax
from jax.experimental import pallas as pl
from jax.experimental.pallas import tpu as pltpu
from jax.sharding import PartitionSpec as P

MESH = pl.DeviceIdType.MESH
F32 = jnp.float32
BF16 = jnp.bfloat16


def fused(n, nt, x_hbm, y_hbm, w_hbm, sw_hbm, tw_hbm, out, loss_out,
          x_ref, y_ref, w_ref, wf, tw, tg, sp, spx, ssum, srr, tacc, tpx, stat, gap, wcol, lossb, acc,
          lc, wz_s, wz_r, wt_s, wt_r, th_s, th_r, px_s, px_r, rs_s, rs_r,
          st_s, st_r, gz_s, gz_r, gx_s, gx_r, ls_s, ls_r):
    z = lax.axis_index("voc")
    t = lax.axis_index("tok")
    h = lax.axis_index("hid")
    rows, ks = x_ref.shape
    kt = y_ref.shape[1]
    half = rows // 2
    quarter = ks // nt
    partner = {"hid": 1 - h}
    mine = pl.ds(pl.multiple_of(h * half, half), half)
    theirs = pl.ds(pl.multiple_of((1 - h) * half, half), half)
    me = t * 2 + h

    def rc(src, dst, ss, rs, dev):
        return pltpu.make_async_remote_copy(
            src_ref=src, dst_ref=dst, send_sem=ss, recv_sem=rs,
            device_id=dev, device_id_type=MESH)

    def zdev(k):
        return lax.rem(z + k, n)

    plane = []
    for q in range(nt):
        for c in range(2):
            if q or c:
                plane.append((lax.rem(t + q, nt), lax.rem(h + c, 2)))

    own_w = pltpu.make_async_copy(sw_hbm.at[pl.ds(pl.multiple_of(z * ks, ks), ks)], wf.at[z], lc.at[n])
    own_w.start()
    ins = [pltpu.make_async_copy(a, b, lc.at[n + 1 + i])
           for i, (a, b) in enumerate(((x_hbm, x_ref), (y_hbm, y_ref), (w_hbm, w_ref)))]
    for c in ins:
        c.start()

    def tw_copy(i):
        return pltpu.make_async_copy(tw_hbm.at[pl.ds(pl.multiple_of(i * kt, kt), kt)], tw.at[i], lc.at[i])

    barrier = pltpu.get_barrier_semaphore()
    for k in range(1, n):
        pl.semaphore_signal(barrier, inc=1, device_id={"voc": zdev(k)}, device_id_type=MESH)
    for (a, b) in plane:
        pl.semaphore_signal(barrier, inc=1, device_id={"tok": a, "hid": b}, device_id_type=MESH)
    pl.semaphore_wait(barrier, n - 1 + len(plane))

    def part(i):
        return pl.ds(pl.multiple_of(i * quarter, quarter), quarter)

    def wz(j):
        return rc(sw_hbm.at[pl.ds(pl.multiple_of(j * ks + t * quarter, quarter), quarter)],
                  wf.at[z, part(t)], wz_s.at[j], wz_r.at[z], {"voc": j})

    def wz_in(j):
        return rc(wf.at[j, part(t)], wf.at[j, part(t)], wz_s.at[j], wz_r.at[j], {"voc": j})

    def wt(j, dst_t):
        return rc(wf.at[j, part(t)], wf.at[j, part(t)], wt_s.at[j, dst_t], wt_r.at[j, t], {"tok": dst_t})

    def wt_in(j, src_t):
        return rc(wf.at[j, part(src_t)], wf.at[j, part(src_t)], wt_s.at[j, src_t], wt_r.at[j, src_t], {"tok": src_t})

    def sides(d):
        return ((z - d, z - d >= 0), (z + d, z + d < n))

    for d in range(n - 1, 0, -1):
        for j, ok in sides(d):
            @pl.when(ok)
            def _(j=j):
                wz(j).start()

    def piece(r):
        return pl.ds(r * half, half)

    def own_y(r, side):
        return rc(y_hbm.at[piece(r)], tg.at[z, piece(r)], th_s.at[side, z, r], th_r.at[z, r],
                  {"voc": z + (1 if side else -1)})

    def relay_y(i, r, side):
        return rc(tg.at[i, piece(r)], tg.at[i, piece(r)], th_s.at[side, i, r], th_r.at[i, r],
                  {"voc": z + (1 if side else -1)})

    room = (z - 1 >= 0, z + 1 < n)
    for r in range(2):
        for side in range(2):
            @pl.when(room[side])
            def _(r=r, side=side):
                own_y(r, side).start()

    for k in range(n):
        tw_copy(zdev(k)).start()

    for c in ins:
        c.wait()
    wcol[...] = jnp.transpose(jnp.broadcast_to(w_ref[...], (rows, rows)))

    for d in range(n - 1, 0, -1):
        for j, ok in sides(d):
            @pl.when(ok)
            def _(j=j):
                wz_in(j).wait_recv()
                for q in range(1, nt):
                    wt(j, lax.rem(t + q, nt)).start()

    def teacher_dot(src, i, first):
        tw_copy(i).wait()
        step = kt // 2

        @pl.loop(0, 2)
        def _(s):
            cols = pl.ds(pl.multiple_of(s * step, step), step)
            term = jnp.dot(src[:, cols], tw[i, cols, :], preferred_element_type=F32)
            if first:
                @pl.when(s == 0)
                def _():
                    tacc[...] = term

                @pl.when(s > 0)
                def _():
                    tacc[...] += term
            else:
                tacc[...] += term

    teacher_dot(y_ref, z, True)

    def take_y(d, dot):
        for r in range(2):
            for side, (i, ok) in enumerate(sides(d)):
                @pl.when(ok)
                def _(i=i, side=side, r=r):
                    relay_y(i, r, side).wait_recv()
                    if d < n - 1:
                        on = 1 - side

                        @pl.when(room[on])
                        def _():
                            relay_y(i, r, on).start()
        if dot:
            dot_y(d)

    def dot_y(d):
        for i, ok in sides(d):
            @pl.when(ok)
            def _(i=i):
                teacher_dot(tg.at[i], i, False)

    def student(j, own):
        if own:
            own_w.wait()
        else:
            for q in range(1, nt):
                wt_in(j, lax.rem(t + q, nt)).wait_recv()
        sp[j] = jnp.dot(x_ref[...], wf[j], preferred_element_type=F32)
        swap = rc(sp.at[j, theirs], spx.at[j], px_s.at[j], px_r.at[j], partner)
        swap.start()
        swap.wait_recv()
        ssum[j] = sp[j, mine, :] + spx[j]

    def rs(side, j):
        return rc(ssum.at[j], srr.at[side, j], rs_s.at[j], rs_r.at[side, j],
                  {"voc": z + (1 if side else -1)})

    def student_step(d):
        for side, (j, ok) in enumerate(sides(d)):
            @pl.when(ok)
            def _(j=j, side=side):
                student(j, False)

                @pl.when(room[1 - side])
                def _():
                    rs(side, j).wait_recv()
                    ssum[j] += srr[side, j]
                rs(side, j).start()

    take_y(1, False)
    student_step(n - 1)
    dot_y(1)
    for d in range(n - 2, 0, -1):
        if d == 1:
            for e in range(2, n - 1):
                take_y(e, True)
        student_step(d)
    student(z, True)
    for side in range(2):
        @pl.when(room[1 - side])
        def _(side=side):
            rs(side, z).wait_recv()
            ssum[z] += srr[side, z]
    sl = ssum[z]
    ms = jnp.max(sl, axis=1, keepdims=True)
    ss = jnp.sum(jnp.exp(sl - ms), axis=1, keepdims=True)
    take_y(n - 1, True)

    tx = rc(tacc.at[theirs], tpx, px_s.at[n], px_r.at[n], partner)
    tx.start()
    tx.wait_recv()
    tl = tacc[mine, :] + tpx[...]
    tpx[...] = tl
    mt = jnp.max(tl, axis=1, keepdims=True)
    et = jnp.exp(tl - mt)
    st = jnp.sum(et, axis=1, keepdims=True)
    cr = jnp.sum(et * (tl - sl), axis=1, keepdims=True)
    lane = lax.broadcasted_iota(jnp.int32, (half, 128), 1)
    cols = jnp.where(lane == 0, ms, jnp.where(lane == 1, mt, jnp.where(
        lane == 2, ss, jnp.where(lane == 3, st, cr))))
    stat[z] = jnp.transpose(jnp.concatenate([cols] * (128 // half), axis=0))[:8]

    def stx(j, src):
        return rc(stat.at[src], stat.at[src], st_s.at[j], st_r.at[src], {"voc": j})

    for k in range(1, n):
        stx(zdev(k), z).start()
    for k in range(1, n):
        stx(zdev(k), zdev(k)).wait_recv()
    parts = [stat[j] for j in range(n)]
    top = parts[0]
    for p in parts[1:]:
        top = jnp.maximum(top, p)
    big_s, big_t = top[0:1], top[1:2]
    tot_s = jnp.zeros_like(big_s)
    tot_t = jnp.zeros_like(big_s)
    cross = jnp.zeros_like(big_s)
    for p in parts:
        es = jnp.exp(p[0:1] - big_s)
        ets = jnp.exp(p[1:2] - big_t)
        tot_s = tot_s + p[2:3] * es
        tot_t = tot_t + p[3:4] * ets
        cross = cross + p[4:5] * ets
    lse_s = big_s + jnp.log(tot_s)
    lse_t = big_t + jnp.log(tot_t)
    scale = wcol[mine, :][:, 0:1]
    sub = lax.broadcasted_iota(jnp.int32, (128, 128), 0)
    back = jnp.transpose(jnp.where(sub == 0, lse_s, lse_t))[:half]
    col_s, col_t = back[:, 0:1], back[:, 1:2]
    gap[z, mine, :] = (scale * (jnp.exp(ssum[z] - col_s) - jnp.exp(tpx[...] - col_t))).astype(BF16)

    def gz(j, src):
        return rc(gap.at[src, mine], gap.at[src, mine], gz_s.at[j], gz_r.at[src], {"voc": j})

    def gx(src, side):
        return rc(gap.at[src, side], gap.at[src, side], gx_s.at[src], gx_r.at[src], partner)

    for d in range(1, n):
        for j, ok in sides(d):
            @pl.when(ok)
            def _(j=j):
                gz(j, z).start()
    gx(z, mine).start()

    div = cross / tot_t - lse_t + lse_s
    first = lax.broadcasted_iota(jnp.int32, div.shape, 1) < half
    lossb[me] = jnp.broadcast_to(jnp.sum(jnp.where(first, div, 0.0), axis=1, keepdims=True), (8, 128))

    def ls(a, b, src):
        return rc(lossb.at[src], lossb.at[src], ls_s.at[a * 2 + b], ls_r.at[src], {"tok": a, "hid": b})

    for (a, b) in plane:
        ls(a, b, me).start()

    def grad_dot(j, first):
        term = lax.dot_general(gap[j], wf[j], (((1,), (1,)), ((), ())), preferred_element_type=F32)
        if first:
            acc[...] = term
        else:
            acc[...] += term

    gx(z, theirs).wait_recv()
    grad_dot(z, True)
    for d in range(1, n):
        for j, ok in sides(d):
            @pl.when(ok)
            def _(j=j):
                gz(j, j).wait_recv()
                gx(j, mine).start()
    for k in range(1, n):
        j = zdev(k)
        gx(j, theirs).wait_recv()
        grad_dot(j, False)
    out[...] = acc[...].astype(BF16)

    for (a, b) in plane:
        ls(a, b, a * 2 + b).wait_recv()
    total = lossb[0]
    for p in range(1, nt * 2):
        total = total + lossb[p]
    loss_out[0, 0] = total[0, 0] / (rows * nt)

    for k in range(1, n):
        j = zdev(k)
        wz(j).wait_send()
        for q in range(1, nt):
            wt(j, lax.rem(t + q, nt)).wait_send()
        rc(ssum.at[j], srr.at[0, j], rs_s.at[j], rs_r.at[0, j], {"voc": j}).wait_send()
        stx(j, z).wait_send()
        gz(j, z).wait_send()
    for r in range(2):
        for side in range(2):
            @pl.when(room[side])
            def _(r=r, side=side):
                own_y(r, side).wait_send()
    for d in range(1, n - 1):
        for r in range(2):
            for side, (i, ok) in enumerate(sides(d)):
                on = 1 - side

                @pl.when(jnp.logical_and(ok, room[on]))
                def _(i=i, r=r, on=on):
                    relay_y(i, r, on).wait_send()
    for k in range(n):
        j = zdev(k)
        rc(sp.at[j, theirs], spx.at[j], px_s.at[j], px_r.at[j], partner).wait_send()
        gx(j, mine).wait_send()
    tx.wait_send()
    for (a, b) in plane:
        ls(a, b, me).wait_send()


def fused_shards(n, nt, student_hidden, teacher_hidden, student_head, teacher_head, loss_weight):
    rows, ks = student_hidden.shape
    kt = teacher_hidden.shape[1]
    v = student_head.shape[1]
    half = rows // 2
    dma = lambda *s: pltpu.SemaphoreType.DMA(s)
    vmem = lambda s, d: pltpu.VMEM(s, d)
    whole = pl.BlockSpec(memory_space=pltpu.VMEM)
    anywhere = pl.BlockSpec(memory_space=pl.ANY)
    grad, loss = pl.pallas_call(
        functools.partial(fused, n, nt),
        out_shape=(jax.ShapeDtypeStruct((rows, ks), BF16), jax.ShapeDtypeStruct((1, 1), F32)),
        in_specs=[anywhere] * 5,
        out_specs=(whole, pl.BlockSpec(memory_space=pltpu.SMEM)),
        scratch_shapes=[
            vmem((rows, ks), BF16),
            vmem((rows, kt), BF16),
            vmem((1, rows), F32),
            vmem((n, ks, v), BF16),
            vmem((n, kt, v), BF16),
            vmem((n, rows, kt), BF16),
            vmem((n, rows, v), F32),
            vmem((n, half, v), F32),
            vmem((n, half, v), F32),
            vmem((2, n, half, v), F32),
            vmem((rows, v), F32),
            vmem((half, v), F32),
            vmem((n, 8, 128), F32),
            vmem((n, rows, v), BF16),
            vmem((rows, rows), F32),
            vmem((nt * 2, 8, 128), F32),
            vmem((rows, ks), F32),
            dma(n + 4),
            dma(n), dma(n), dma(n, nt), dma(n, nt),
            dma(2, n, 2), dma(n, 2),
            dma(n + 1), dma(n + 1), dma(n), dma(2, n),
            dma(n), dma(n), dma(n), dma(n), dma(n), dma(n),
            dma(nt * 2), dma(nt * 2),
        ],
        compiler_params=pltpu.CompilerParams(
            collective_id=0, has_side_effects=True, vmem_limit_bytes=60 << 20),
        name="divergence_grad",
    )(student_hidden, teacher_hidden, loss_weight.reshape(1, rows), student_head, teacher_head)
    return grad, loss.reshape(())


def divergence_terms(student_logits, teacher_logits, weights):
    differences = teacher_logits - student_logits
    peak_student, peak_teacher = lax.pmax(
        (jnp.max(student_logits, axis=1), jnp.max(teacher_logits, axis=1)), "voc"
    )
    scaled_student = jnp.exp(student_logits - peak_student[:, None])
    scaled_teacher = jnp.exp(teacher_logits - peak_teacher[:, None])
    total_student, total_teacher, cross_sum = lax.psum(
        (
            jnp.sum(scaled_student, axis=1),
            jnp.sum(scaled_teacher, axis=1),
            jnp.sum(scaled_teacher * differences, axis=1),
        ),
        "voc",
    )
    student_lse = peak_student + jnp.log(total_student)
    teacher_lse = peak_teacher + jnp.log(total_teacher)
    divergence = cross_sum / total_teacher - teacher_lse + student_lse
    prob_gap = jnp.exp(student_logits - student_lse[:, None]) - jnp.exp(
        teacher_logits - teacher_lse[:, None]
    )
    scaled_gap = (weights[:, None] * prob_gap).astype(jnp.bfloat16)
    return (divergence, scaled_gap)


def plain_shards(student_hidden, teacher_hidden, student_head, teacher_head, loss_weight):
    student_block, teacher_block = (
        lax.all_gather(student_hidden, "voc", axis=1, tiled=True),
        lax.all_gather(teacher_hidden, "voc", axis=1, tiled=True),
    )
    vocab_local = student_head.shape[1]
    row_count = student_block.shape[0] // lax.axis_size("hid")
    joined = lax.psum_scatter(
        jnp.concatenate(
            [
                jnp.dot(student_block, student_head, preferred_element_type=jnp.float32),
                jnp.dot(teacher_block, teacher_head, preferred_element_type=jnp.float32),
            ],
            axis=1,
        ),
        "hid",
        scatter_dimension=0,
        tiled=True,
    )
    student_logits = joined[:, :vocab_local]
    teacher_logits = joined[:, vocab_local:]
    weights = lax.dynamic_slice_in_dim(loss_weight, lax.axis_index("hid") * row_count, row_count)
    divergence, scaled_gap = divergence_terms(student_logits, teacher_logits, weights)
    token_total = loss_weight.shape[0] * lax.axis_size("tok")
    loss_total = lax.psum(jnp.sum(divergence), ("tok", "hid"))
    grad_terms = lax.dot_general(
        lax.all_gather(scaled_gap, "hid", axis=0, tiled=True),
        student_head,
        (((1,), (1,)), ((), ())),
        preferred_element_type=jnp.float32,
    )
    grad_hidden = lax.psum_scatter(grad_terms, "voc", scatter_dimension=1, tiled=True).astype(
        jnp.bfloat16
    )
    mean_loss = loss_total / token_total
    return (grad_hidden, mean_loss)


def solution(mesh):
    placed = (
        P("tok", ("hid", "voc")),
        P("tok", ("hid", "voc")),
        P("hid", "voc"),
        P("hid", "voc"),
        P("tok"),
    )
    n, nt = mesh.shape["voc"], mesh.shape["tok"]
    if 2 < n <= 4 and mesh.shape["hid"] == 2:
        body = functools.partial(fused_shards, n, nt)
    else:
        body = plain_shards
    return jax.shard_map(
        body,
        mesh=mesh,
        in_specs=placed,
        out_specs=(P("tok", ("hid", "voc")), P()),
        check_vma=False,
    )
```
